32 devices in a mesh: ice: 4 (over x, core), ocn: 8 (over z, y).
Axes of the slice: x: 2, y: 2, z: 4, core: 2. Of those that a mesh axis runs over, the one named last changes fastest.
Arguments:
- ice_state: bfloat16 [5, 20, 32768], P(None, None, ('ice', 'ocn')), may hold values from -6 to 6
- ocean_state: bfloat16 [5, 20, 32768], P(None, None, ('ice', 'ocn')), may hold values from -5 to 5
- ice_rate: float32 [5, 20], replicated, may hold values from 0.2 to 2
- block_weights: bfloat16 [1024, 128, 128], P(('ice', 'ocn')), may hold values from -0.375 to 0.375
- block_route: int32 [1024, 1], P(('ice', 'ocn')), may hold values from 0 to 31; in each aligned block of 32 rows (0 to 31, 32 to 63, ...) at most 2 rows name the same one
- block_tiles: int32 [1024, 2], P(('ice', 'ocn')), may hold values from 0 to 7
- block_valid: int32 [1024], P(('ice', 'ocn')), may hold values from 16 to 128
- ice_mask: int32 [32768], P(('ice', 'ocn')), may hold values 0 or 1
Outputs:
- ice_final: bfloat16 [5, 20, 32768], P(None, None, ('ice', 'ocn'))
- ocean_flux: bfloat16 [5, 20, 32768], P(None, None, ('ice', 'ocn'))
The draws below stay inside these ranges and needn't reach their ends.
Inputs may be any that keep to these rules, and one draw needn't show every extreme that they name: `block_route`: among the blocks of one device no destination appears more than 2 times.
All inputs are finite; a program needn't handle non-finite values. No bound on the sum of `ice_mask` on one device may be relied on, other than what follows from the above.
Results may differ from the reference program's by a relative error of at most 0.008.
Values may be sent and summed in bfloat16 or wider, within the bound.
A program may use at most 128 MiB of HBM per device.

```python
import math
import jax
import jax.numpy as jnp
import numpy as np
from jax import lax

CATS = 5
FIELDS = 20
BLOCK = 128
CAP = 2
TILES = 8
NB = 32
NI = 32768
NO = 32768
DEVICES = 32


def with_ends(values, stream_key, low, top_value):
    place = [jax.random.randint(jax.random.fold_in(stream_key, axis), (), 0, length) for axis, length in enumerate(values.shape)]
    widest = values.shape.index(max(values.shape))
    next_to = place[:widest] + [(place[widest] + 1) % values.shape[widest]] + place[widest + 1:]
    return values.at[tuple(place)].set(low).at[tuple(next_to)].set(top_value)


def levels(rng, extent, pieces, low, high):
    def one(position, shards_of):
        draws = jax.random.uniform(jax.random.fold_in(jax.random.fold_in(rng, 6), position), (shards_of,), jnp.float32, low / len(pieces), high / len(pieces))
        return jnp.repeat(jnp.exp(draws), extent[position] // shards_of).reshape((-1,) + (1,) * (len(extent) - position - 1))

    gain = one(*pieces[0])
    for cut in pieces[1:]:
        gain = gain * one(*cut)
    return gain


def routed_block(own_key, own, number, rows, count, top, reach, slope):
    ranking = jax.random.permutation(own_key, count)
    packed, ordinary = shares(count, rows * top, reach, slope, True), shares(count, rows * top, reach, slope, False)
    places = jnp.arange(count)

    def named(lengths, turn):
        used = int((lengths > 0).sum())
        fixed = max(1, used // 4)
        shifted = fixed + (places - fixed + turn * (used - fixed)) % max(1, count - fixed)
        return jnp.zeros((count,), jnp.int32).at[ranking[jnp.where(places < fixed, places, shifted)]].set(jnp.asarray(lengths, jnp.int32))

    lengths = jnp.where(number % 4 == 0, named(packed, number // 4), named(ordinary, number - number // 4 - 1))
    mixed = jax.random.permutation(jax.random.fold_in(own, 3), count)
    donor, receiver = mixed[0:count // 2 * 2:2], mixed[1:count // 2 * 2:2]
    slack = jnp.minimum(lengths[donor] - 1, reach - lengths[receiver]) // 2
    slack = jnp.where((donor == ranking[0]) | (receiver == ranking[0]) | (lengths[receiver] == 0), 0, jnp.maximum(slack, 0))
    shifted = jax.random.randint(jax.random.fold_in(own, 4), (count // 2,), 0, 1 << 20) % (slack + 1)
    lengths = lengths.at[donor].add(-shifted).at[receiver].add(shifted)
    members = jnp.searchsorted(jnp.cumsum(lengths), jnp.arange(rows * top), side="right").astype(jnp.int32)
    listing = members.reshape(top, rows).T
    listing = listing[jax.random.permutation(jax.random.fold_in(own, 1), rows)]
    turn = jax.random.randint(jax.random.fold_in(own, 2), (rows, 1), 0, top)
    return jnp.take_along_axis(listing, (jnp.arange(top)[None, :] + turn) % top, axis=1)


def shares(amount, total, limit, slope, full):
    weights = [(1 << 20) // math.isqrt(standing ** slope) + 1 for standing in range(1, amount + 1)]
    largest = limit if full else min(limit, max(-(-total // amount), total * weights[0] // sum(weights)))
    least = 1 if total - largest >= amount - 1 else 0
    holding, rest = [largest] + [least] * (amount - 1), total - largest - least * (amount - 1)
    while rest > 0:
        free = [i for i in range(1, amount) if holding[i] < largest] or [i for i in range(1, amount) if holding[i] < limit]
        whole, left = sum([weights[i] for i in free]), rest
        for i in free:
            addition = min(limit - holding[i], max(1, left * weights[i] // whole), rest)
            holding[i] = holding[i] + addition
            rest = rest - addition
    return np.array(holding)


def normal_values(own_key, shape, deviation, reach, pieces=(), held_as=jnp.bfloat16):
    array = deviation * jax.random.normal(own_key, shape, jnp.float32)
    if pieces:
        array = array * levels(own_key, shape, pieces, -0.22, 0.18)
    return jnp.clip(array, -reach, reach).astype(held_as)


def setup_inputs(seed: int = 0) -> dict:
    streams_of = jax.random.split(jax.random.key(seed), 9)
    ice_state = normal_values(streams_of[0], (CATS, FIELDS, NI), 1.0, 6.0, ((2, 32),))
    ocean_state = normal_values(streams_of[1], (CATS, FIELDS, NO), 0.7, 5.0, ((2, 32),))
    ice_rate = jnp.clip(jnp.exp(jax.random.uniform(streams_of[2], (CATS, FIELDS), jnp.float32, math.log(0.2), math.log(2.0))), 0.2, 2.0)
    block_weights = normal_values(streams_of[3], (NB * DEVICES, BLOCK, BLOCK), (NB * BLOCK // (2 * TILES)) ** -0.5, 0.375, ((0, 32),))
    block_route_keys = jax.random.split(jax.random.fold_in(streams_of[4], 1), (NB * DEVICES) // NB)
    block_route_turns = jax.random.permutation(jax.random.fold_in(streams_of[4], 3), (NB * DEVICES) // NB)
    block_route = jax.vmap(lambda own, number: routed_block(jax.random.fold_in(streams_of[4], 2), own, number, NB, DEVICES, 1, CAP, 1))(block_route_keys, block_route_turns).reshape((NB * DEVICES, 1))
    block_tiles = with_ends(jax.random.randint(streams_of[5], (NB * DEVICES, 2), 0, TILES), jax.random.fold_in(streams_of[5], 1), 0, TILES - 1).astype(jnp.int32)
    block_valid = with_ends(jax.random.randint(streams_of[6], (NB * DEVICES,), BLOCK // 8, BLOCK + 1), jax.random.fold_in(streams_of[6], 1), BLOCK // 8, BLOCK).astype(jnp.int32)
    ice_mask = with_ends((jax.random.randint(streams_of[7], (NI,), 0, 4) < 3).astype(jnp.int32), jax.random.fold_in(streams_of[7], 1), 0, 1)
    return {"ice_state": ice_state, "ocean_state": ocean_state, "ice_rate": ice_rate, "block_weights": block_weights, "block_route": block_route, "block_tiles": block_tiles, "block_valid": block_valid, "ice_mask": ice_mask}


def reference(ice_state, ocean_state, ice_rate, block_weights, block_route, block_tiles, block_valid, ice_mask):
    chans = CATS * FIELDS
    live = jnp.arange(BLOCK, dtype=jnp.int32)[None, :] < block_valid[:, None]
    masked = jnp.where(live[:, :, None], block_weights, jnp.zeros((), jnp.bfloat16)).reshape(DEVICES, NB, BLOCK, BLOCK)
    route = block_route[:, 0].reshape(DEVICES, NB)
    source = block_tiles[:, 0].reshape(DEVICES, NB)
    target = (route * TILES + block_tiles[:, 1].reshape(DEVICES, NB)).astype(jnp.int32)
    rates = ice_rate.reshape(chans, 1).astype(jnp.float32)
    land = ice_mask.astype(jnp.float32)[None, :]
    ocean = ocean_state.reshape(chans, NO).astype(jnp.float32)
    ice = (ice_state * ice_mask.astype(jnp.bfloat16)[None, None, :]).reshape(chans, NI)
    flux = None
    for turn in range(2):
        tiles_all = jnp.transpose(ice.reshape(chans, DEVICES, TILES, BLOCK), (1, 0, 2, 3))

        def forward(acc, item):
            tile_set, weights, picks, places = item
            picked = tile_set[:, picks, :].astype(jnp.float32)
            prods = jnp.einsum("cbi,bio->bco", picked, weights.astype(jnp.float32)).astype(jnp.bfloat16)
            prods = lax.optimization_barrier(prods).astype(jnp.float32)
            return acc.at[places].add(prods), None

        start = jnp.zeros((DEVICES * TILES, chans, BLOCK), jnp.float32)
        ocean_in, unused = lax.scan(forward, start, (tiles_all, masked, source, target))
        ocean_in = jnp.transpose(ocean_in, (1, 0, 2)).reshape(chans, NO)
        flux = jnp.tanh(ocean_in + ocean).astype(jnp.bfloat16)
        flux_tiles = jnp.transpose(flux.reshape(chans, DEVICES * TILES, BLOCK), (1, 0, 2))

        def backward(carry, item):
            weights, picks, places = item
            taken = flux_tiles[places].astype(jnp.float32)
            contrib = jnp.einsum("bco,bio->bci", taken, weights.astype(jnp.float32))
            forced = jnp.zeros((TILES, chans, BLOCK), jnp.float32).at[picks].add(contrib)
            return carry, forced

        unused, forcing = lax.scan(backward, jnp.float32(0.0), (masked, source, target))
        forcing = jnp.transpose(forcing, (2, 0, 1, 3)).reshape(chans, NI)
        ice = (land * (ice.astype(jnp.float32) + rates * jnp.tanh(forcing))).astype(jnp.bfloat16)
    return ice.reshape(CATS, FIELDS, NI), flux.reshape(CATS, FIELDS, NO)
```

```python
import functools

import jax
import jax.numpy as jnp
from jax import lax
from jax.experimental import pallas as pl
from jax.experimental.pallas import tpu as pltpu
from jax.sharding import PartitionSpec as P

CAP = 2
CORES = 2
LINE = 4
LANES = 128
AXES = ("ice", "ocn")
SPAN = 256


def order(count, calls):
    steps = []
    for h in range(count):
        for place, call in zip((0, 1, 5, 7, 12, 16, 22), calls):
            steps.append((3 * h + place, h, call))
    return [step[1:] for step in sorted(steps, key=lambda step: step[:2])]


def kernel(
    sizes, parts,
    route_ref, tiles_ref, valid_ref, rate_ref, land_hbm, ice_hbm, ocean_hbm, w_hbm,
    ice_out, flux_out,
    w_in, wsend, wall, tabv, tabs, namv, nams, rates, res, fres, sea, psend, prec,
    ice_g, fb, own, dsend, drec, zsend, zrec, zrel, csend, crec, mine,
    wl, tl, nl, ns_s, ns_r, ws_s, ws_r, ps_s, ps_r, as_s, as_r, ds_s, ds_r, zs_s, zs_r, rl_s, rl_r,
    fs_s, fs_r, fr_s, gs_s, gs_r, cs_s, cs_r, land_ref, ice_in, ocean_in, il,
):
    X, Y, Z, tiles, blocks = sizes
    Q = X * Y
    H = len(parts)
    per = CORES * CAP
    slots = Z * per
    outer = Z * Y
    cats, fields = rate_ref.shape
    ice_id, ocn_id = lax.axis_index("ice"), lax.axis_index("ocn")
    x, c = ice_id // CORES, ice_id % CORES
    z, y = ocn_id // Y, ocn_id % Y
    side = z // (Z // 2)
    zord = ((Z - 1) * (1 - side), Z // 2 - side, z + 1 - 2 * (z % 2), z)
    is_end = z == (Z - 1) * side
    is_mid = z != (Z - 1) * side

    def chip(j, back=False):
        dx, dy = j // Y, j % Y
        if back:
            dx, dy = X - dx, Y - dy
        return {"ice": ((x + dx) % X) * CORES + c, "ocn": z * Y + (y + dy) % Y}

    partner = {"ice": x * CORES + 1 - c, "ocn": ocn_id}

    def line(zt):
        return {"ice": ice_id, "ocn": zt * Y + y}

    def remote(src, dst, s, r, dev):
        return pltpu.make_async_remote_copy(
            src_ref=src, dst_ref=dst, send_sem=s, recv_sem=r,
            device_id=dev, device_id_type=pl.DeviceIdType.MESH,
        )

    wload = pltpu.make_async_copy(w_hbm, w_in, wl)
    loads = [
        pltpu.make_async_copy(src, dst, il.at[i])
        for i, (src, dst) in enumerate(((land_hbm, land_ref), (ice_hbm, ice_in), (ocean_hbm, ocean_in)))
    ]
    for load in loads:
        load.start()
    wload.start()

    hops = {j: min(j // Y, X - j // Y) + min(j % Y, Y - j % Y) for j in range(Q)}
    near = sorted(range(1, Q), key=hops.get)

    barrier = pltpu.get_barrier_semaphore()
    for j in range(1, Q):
        pl.semaphore_signal(barrier, inc=1, device_id=chip(j), device_id_type=pl.DeviceIdType.MESH)
    for i in range(1, Z):
        pl.semaphore_signal(barrier, inc=1, device_id=line((z + i) % Z), device_id_type=pl.DeviceIdType.MESH)
    pl.semaphore_signal(barrier, inc=1, device_id=partner, device_id_type=pl.DeviceIdType.MESH)

    def acopy(h, j):
        return remote(ice_g[h].at[0], ice_g[h].at[j], as_s.at[h, j], as_r.at[h, j], chip(j))

    def ncopy(j):
        return remote(namv.at[j], namv.at[Q + j], ns_s.at[j], ns_r.at[j], chip(j))

    def wcopy(j):
        return remote(wsend.at[j], wall.at[j], ws_s.at[j], ws_r.at[j], chip(j))

    def pcopy(h, g, j):
        at = pl.ds(zord[g] * per, per)
        return remote(psend[h].at[j, at], prec[h].at[j, at], ps_s.at[h, g, j], ps_r.at[h, g, j], chip(j))

    def dcopy(h, zd):
        return remote(dsend[h].at[zd], drec[h].at[zd], ds_s.at[h, zd], ds_r.at[h, zd], partner)

    def zcopy(h, zd):
        return remote(zsend[h].at[zd], zrec[h].at[z], zs_s.at[h, zd], zs_r.at[h, z], line(zd))

    def zwait(h, zs):
        remote(zsend[h].at[zs], zrec[h].at[zs], zs_s.at[h, zs], zs_r.at[h, zs], line(zs)).wait_recv()

    def rcopy(h, g):
        return remote(zsend[h].at[zord[g]], zrel[h].at[g], rl_s.at[h, g], rl_r.at[h, g], line(zord[2]))

    def fcopy(h, zt):
        return remote(fb[h].at[c, z], fb[h].at[c, z], fs_s.at[h, zt], fs_r.at[h, z], line(zt))

    def fwait(h, zs):
        remote(fb[h].at[c, zs], fb[h].at[c, zs], fs_s.at[h, zs], fs_r.at[h, zs], line(zs)).wait_recv()

    def frelay(h, g):
        held = fb[h].at[c, zord[g]]
        return remote(held, held, fr_s.at[h, g], fs_r.at[h, zord[g]], line(zord[2]))

    def gcopy(h, zs):
        return remote(fb[h].at[c, zs], fb[h].at[c, zs], gs_s.at[h, zs], gs_r.at[h, zs], partner)

    def gwait(h, zs):
        held = fb[h].at[1 - c, zs]
        remote(held, held, gs_s.at[h, zs], gs_r.at[h, zs], partner).wait_recv()

    def ccopy(h, j):
        return remote(csend[h].at[j], crec[h].at[j], cs_s.at[h, j], cs_r.at[h, j], chip(j, True))

    def lanes(t):
        return pl.ds(t * LANES, LANES)

    def land(t):
        return land_ref[pl.ds(t, 1), :].astype(jnp.float32)

    tall = -(-Q // 8) * 8
    sub = lax.broadcasted_iota(jnp.int32, (tall, LANES), 0)
    lane = lax.broadcasted_iota(jnp.int32, (tall, LANES), 1)
    base = jnp.zeros((tall, LANES), jnp.int32)
    for j in range(Q):
        dx, dy = j // Y, j % Y
        own_base = ((x + dx) % X) * CORES * outer + (y + dy) % Y
        base = jnp.where(sub == j, own_base, base)
    turn_of = lane & (CAP - 1)
    core_of = lax.shift_right_logical(lane, CAP.bit_length() - 1) & (CORES - 1)
    line_of = lax.shift_right_logical(lane, per.bit_length() - 1)
    dest = base + core_of * outer + line_of * Y

    def enter(b, carry):
        seen, code, name = carry
        hit = dest == route_ref[0, b]
        take = hit & (seen == turn_of)
        label = tiles_ref[0, b] * tiles + tiles_ref[1, b]
        code = jnp.where(take, (b * SPAN + valid_ref[b]) * (tiles * tiles) + label, code)
        name = jnp.where(take, label, name)
        return seen + jnp.where(hit, 1, 0), code, name

    none = jnp.zeros((tall, LANES), jnp.int32)
    unused, code, name = lax.fori_loop(0, blocks, enter, (none, none, none), unroll=8)
    for j in range(Q):
        tabv[j] = code[j : j + 1, :]
        namv[j] = name[j : j + 1, :]
    tload = pltpu.make_async_copy(tabv, tabs, tl)
    tload.start()

    for load in loads:
        load.wait()
    chans, padded = cats * fields, rates.shape[0]
    for t in range(tiles):
        if chans < padded:
            spare = jnp.zeros((8, LANES), jnp.float32)
            res[t, pl.ds(padded - 8, 8), :] = spare
            sea[t, pl.ds(padded - 8, 8), :] = spare
        for r in range(cats):
            at = pl.ds(r * fields, fields)
            res[t, at, :] = ice_in[r, :, lanes(t)].astype(jnp.float32) * land(t)
            sea[t, at, :] = ocean_in[r, :, lanes(t)].astype(jnp.float32)
    if chans < padded:
        rates[pl.ds(padded - 8, 8), :] = jnp.zeros((8, LANES), jnp.float32)
    for h, (first, count) in enumerate(parts):
        for t in range(tiles):
            ice_g[h][0, t] = res[t, pl.ds(first, count), :].astype(jnp.bfloat16)

    pl.semaphore_wait(barrier, Q - 1 + Z - 1 + 1)
    for j in range(1, Q):
        ncopy(j).start()
    nload = [
        pltpu.make_async_copy(namv.at[j if j == 0 else Q + j], nams.at[j], nl.at[j]) for j in range(Q)
    ]
    nload[0].start()
    tload.wait()
    wload.wait()

    rows = lax.broadcasted_iota(jnp.int32, (LANES, LANES), 0)

    def block(j, n):
        v = tabs[j, 0, n] // (tiles * tiles)
        held = w_in[v // SPAN]
        return jnp.where(rows < v % SPAN, held, jnp.zeros((), jnp.bfloat16))

    def products(h, j, n, held):
        v = tabs[j, 0, n] % (tiles * tiles)
        prod = jnp.dot(ice_g[h][0, v // tiles], held, preferred_element_type=jnp.float32)
        return prod.astype(jnp.bfloat16)

    for g in range(Z):
        def put(i, carry):
            j = Q - 1 - i
            for k in range(per):
                n = zord[g] * per + k
                held = block(j, n)
                wsend[j, n] = held
                for h in range(H):
                    psend[h][j, n] = products(h, j, n, held)
            for h in range(H):
                pcopy(h, g, j).start()
            return carry

        lax.fori_loop(0, Q - 1, put, 0)
    for j in near:
        wcopy(j).start()

    def keep(zd, carry):
        for k in range(per):
            n = zd * per + k
            held = block(0, n)
            wall[0, n] = held
            for h in range(H):
                prec[h][0, n] = products(h, 0, n, held)
        return carry

    lax.fori_loop(0, Z, keep, 0)
    for r in range(cats):
        for f in range(fields):
            rates[pl.ds(r * fields + f, 1), :] = jnp.full((1, LANES), rate_ref[r, f], jnp.float32)
    for j in range(1, Q):
        ncopy(j).wait_recv()
        nload[j].start()
    for j in range(Q):
        nload[j].wait()

    def spread(count, index, prod, accs):
        at = jnp.full((count, LANES), index, jnp.int32)
        return tuple(accs[t] + jnp.where(at == t, prod, 0.0) for t in range(tiles))

    def forward(h, zd, ready=False):
        count = parts[h][1]
        start = tuple(jnp.zeros((count, LANES), jnp.float32) for t in range(tiles))

        def sums(core):
            def add(j, accs):
                for k in range(CAP):
                    n = zd * per + core * CAP + k
                    v = nams[j, 0, n]
                    if ready:
                        prod = prec[h][j, n].astype(jnp.float32)
                    else:
                        prod = jnp.dot(ice_g[h][j, v // tiles], wall[j, n], preferred_element_type=jnp.float32)
                    accs = spread(count, v % tiles, prod, accs)
                return accs

            return lax.fori_loop(0, Q, add, start, unroll=min(Q, 4))

        accs = sums(1 - c)
        for t in range(tiles):
            dsend[h][zd, t] = accs[t].astype(jnp.bfloat16)
        dcopy(h, zd).start()
        accs = sums(c)
        for t in range(tiles):
            own[h][zd, t] = accs[t]

    def merge(h, g):
        zd = zord[g]
        dcopy(h, zd).wait_recv()

        def put():
            for t in range(tiles):
                zsend[h][zd, t] = (own[h][zd, t] + drec[h][zd, t].astype(jnp.float32)).astype(jnp.bfloat16)

        if g < 2:
            @pl.when(is_end)
            def _():
                put()
                rcopy(h, g).start()
        elif g == 2:
            put()
            zcopy(h, zd).start()

    def relay(h, which=(0, 1)):
        @pl.when(is_mid)
        def _():
            for g in which:
                zd = zord[g]
                rcopy(h, g).wait_recv()
                for t in range(tiles):
                    acc = own[h][zd, t] + drec[h][zd, t].astype(jnp.float32) + zrel[h][g, t].astype(jnp.float32)
                    zsend[h][zd, t] = acc.astype(jnp.bfloat16)
                zcopy(h, zd).start()

    def flux(h):
        first, count = parts[h]
        zwait(h, zord[2])
        zwait(h, zord[1])
        for t in range(tiles):
            acc = own[h][z, t] + drec[h][z, t].astype(jnp.float32)
            for g in (2, 1):
                acc = acc + zrec[h][zord[g], t].astype(jnp.float32)
            acc = jnp.tanh(acc + sea[t, pl.ds(first, count), :])
            fb[h][c, z, t] = acc.astype(jnp.bfloat16)
            fres[t, pl.ds(first, count), :] = acc

        fcopy(h, zord[1]).start()
        fcopy(h, zord[2]).start()
        gcopy(h, z).start()

    def arrivals(h):
        def take(g):
            fwait(h, zord[g])
            gcopy(h, zord[g]).start()

        @pl.when(is_mid)
        def _():
            for g in (1, 0):
                fwait(h, zord[g])
                frelay(h, g).start()
                gcopy(h, zord[g]).start()
            take(2)

        @pl.when(is_end)
        def _():
            for g in (2, 1, 0):
                take(g)

    def back(h, j):
        count = parts[h][1]
        accs = tuple(jnp.zeros((count, LANES), jnp.float32) for t in range(tiles))
        for n in range(slots):
            zd, core = n // per, n // CAP % CORES
            v = nams[j, 0, n]
            prod = lax.dot_general(
                fb[h][core, zd, v % tiles], wall[j, n], (((1,), (1,)), ((), ())),
                preferred_element_type=jnp.float32,
            )
            accs = spread(count, v // tiles, prod, accs)
        return accs

    def fluxes(h):
        for zs in range(Z):
            gwait(h, zs)

    def give(h, j):
        accs = back(h, j)
        for t in range(tiles):
            csend[h][j, t] = accs[t].astype(jnp.bfloat16)
        ccopy(h, j).start()

    def hold(h):
        accs = back(h, 0)
        for t in range(tiles):
            mine[h][t] = accs[t]

    def backward(h):
        fluxes(h)

        def one(i, carry):
            give(h, Q - 1 - i)
            return carry

        lax.fori_loop(0, Q - 1, one, 0)
        hold(h)

    def finish(h, number):
        first, count = parts[h]
        for j in range(Q - 1, 0, -1):
            ccopy(h, j).wait_recv()
        if number:
            for j in range(1, Q):
                acopy(h, j).wait_send()
        rate = rates[pl.ds(first, count), :]
        for t in range(tiles):
            acc = mine[h][t]
            for j in range(1, Q):
                acc = acc + crec[h][j, t].astype(jnp.float32)
            old = ice_g[h][0, t].astype(jnp.float32)
            new = land(t) * (old + rate * jnp.tanh(acc))
            if number:
                res[t, pl.ds(first, count), :] = new
            else:
                ice_g[h][0, t] = new.astype(jnp.bfloat16)
        if not number:
            for j in range(Q - 1, 0, -1):
                acopy(h, j).start()

        for j in range(1, Q):
            ccopy(h, j).wait_send()
        for zd in range(Z):
            dcopy(h, zd).wait_send()
            gcopy(h, zd).wait_send()
        zcopy(h, zord[2]).wait_send()
        for g in (1, 2):
            fcopy(h, zord[g]).wait_send()

        @pl.when(is_end)
        def _():
            for g in range(2):
                rcopy(h, g).wait_send()

        @pl.when(is_mid)
        def _():
            for g in range(2):
                zcopy(h, zord[g]).wait_send()
                frelay(h, g).wait_send()

    def arrive(h):
        for j in range(Q - 1, 0, -1):
            acopy(h, j).wait_recv()

    def again(h):
        arrive(h)

        def one(zd, carry):
            forward(h, zd)
            return carry

        lax.fori_loop(0, Z, one, 0)

    def merges(h):
        for g in range(Z):
            merge(h, g)

    for g in range(Z):
        for h in range(H):
            for j in range(Q - 1, 0, -1):
                pcopy(h, g, j).wait_recv()
            forward(h, zord[g], True)
        for h in range(H):
            merge(h, g)
        if 0 < g < 3:
            for h in range(H):
                relay(h, (g - 1,))
    for h in range(H):
        flux(h)

    def rest(h):
        def one(i, carry):
            give(h, Q - 1 - i)
            return carry

        fluxes(h)
        lax.fori_loop(0, Q - 1, one, 0)
        hold(h)

    last_near = len(near) - max(1, Q // 4)
    for h in range(2):
        arrivals(h)
    fluxes(0)
    for j in near[:last_near]:
        wcopy(j).wait_recv()
        give(0, j)
    for h in range(2, H):
        arrivals(h)
    for j in near[last_near:]:
        wcopy(j).wait_recv()
        give(0, j)
    hold(0)
    for h in range(1, H):
        rest(h)
        finish(h - 1, 0)
    again(0)
    merges(0)
    finish(H - 1, 0)
    for j in range(1, Q):
        wcopy(j).wait_send()
        ncopy(j).wait_send()
        for h in range(H):
            for g in range(Z):
                pcopy(h, g, j).wait_send()

    def send(r, held, out):
        for t in range(tiles):
            out[r, :, lanes(t)] = held[t, pl.ds(r * fields, fields), :].astype(jnp.bfloat16)

    def last(h):
        if h == H - 1:
            for r in range(cats):
                send(r, fres, flux_out)
        finish(h, 1)
        first, count = parts[h]
        for r in range(cats):
            if first < (r + 1) * fields <= first + count:
                send(r, res, ice_out)

    for h, call in order(H, (again, merges, relay, flux, arrivals, backward, last)):
        if h or call not in (again, merges):
            call(h)


def cut(chans):
    rows = -(-chans // 8) * 8
    sizes = [32] * (rows // 32 - 1)
    sizes.append(rows - sum(sizes))
    parts, first = [], 0
    for size in sizes:
        parts.append((first, size))
        first += size
    return tuple(parts)


def on_device(
    ice_state, ocean_state, ice_rate, block_weights, block_route, block_tiles, block_valid, ice_mask
):
    cats, fields, cells = ice_state.shape
    chans = cats * fields
    blocks, width, unused = block_weights.shape
    tiles = cells // width
    outer = lax.axis_size("ocn")
    Z = LINE
    Y = outer // Z
    X = lax.axis_size("ice") // CORES
    Q = X * Y
    slots = Z * CORES * CAP
    assert outer % LINE == 0
    parts = cut(chans)
    H = len(parts)
    rows = sum(part[1] for part in parts)

    def each(*lead, dtype=jnp.bfloat16):
        return tuple(pltpu.VMEM(lead + (part[1], width), dtype) for part in parts)

    def sems(*shape):
        return pltpu.SemaphoreType.DMA(shape)

    smem, vmem = pl.BlockSpec(memory_space=pltpu.SMEM), pl.BlockSpec(memory_space=pltpu.VMEM)
    ice, flux = pl.pallas_call(
        functools.partial(kernel, (X, Y, Z, tiles, blocks), parts),
        out_shape=(jax.ShapeDtypeStruct(ice_state.shape, jnp.bfloat16),) * 2,
        in_specs=[smem] * 4 + [pl.BlockSpec(memory_space=pltpu.HBM)] * 4,
        out_specs=(vmem, vmem),
        scratch_shapes=[
            pltpu.VMEM((blocks, width, width), jnp.bfloat16),
            pltpu.VMEM((Q, slots, width, width), jnp.bfloat16),
            pltpu.VMEM((Q, slots, width, width), jnp.bfloat16),
            pltpu.VMEM((Q, 1, width), jnp.int32),
            pltpu.SMEM((Q, 1, width), jnp.int32),
            pltpu.VMEM((2 * Q, 1, width), jnp.int32),
            pltpu.SMEM((Q, 1, width), jnp.int32),
            pltpu.VMEM((rows, width), jnp.float32),
            pltpu.VMEM((tiles, rows, width), jnp.float32),
            pltpu.VMEM((tiles, rows, width), jnp.float32),
            pltpu.VMEM((tiles, rows, width), jnp.float32),
            each(Q, slots),
            each(Q, slots),
            each(Q, tiles),
            each(CORES, Z, tiles),
            each(Z, tiles, dtype=jnp.float32),
            each(Z, tiles),
            each(Z, tiles),
            each(Z, tiles),
            each(Z, tiles),
            each(2, tiles),
            each(Q, tiles),
            each(Q, tiles),
            each(tiles, dtype=jnp.float32),
            pltpu.SemaphoreType.DMA,
            pltpu.SemaphoreType.DMA,
            sems(Q), sems(Q), sems(Q),
            sems(Q), sems(Q),
            sems(H, Z, Q), sems(H, Z, Q),
            sems(H, Q), sems(H, Q),
            sems(H, Z), sems(H, Z),
            sems(H, Z), sems(H, Z),
            sems(H, 2), sems(H, 2),
            sems(H, Z), sems(H, Z),
            sems(H, 2),
            sems(H, Z), sems(H, Z),
            sems(H, Q), sems(H, Q),
            pltpu.VMEM((tiles, width), jnp.int32),
            pltpu.VMEM(ice_state.shape, jnp.bfloat16),
            pltpu.VMEM(ice_state.shape, jnp.bfloat16),
            sems(3),
        ],
        compiler_params=pltpu.CompilerParams(
            collective_id=0, has_side_effects=True, vmem_limit_bytes=60 * 1024 * 1024
        ),
    )(
        block_route.T, block_tiles.T, block_valid, ice_rate, ice_mask.reshape(tiles, width),
        ice_state, ocean_state, block_weights,
    )
    return ice, flux


def solution(mesh):
    placed = (
        P(None, None, AXES), P(None, None, AXES), P(), P(AXES, None, None),
        P(AXES, None), P(AXES, None), P(AXES), P(AXES),
    )
    return jax.shard_map(
        on_device, mesh=mesh, in_specs=placed,
        out_specs=(P(None, None, AXES), P(None, None, AXES)), check_vma=False,
    )
```

```python
import functools

import jax
import jax.numpy as jnp
from jax import lax
from jax.experimental import pallas as pl
from jax.experimental.pallas import tpu as pltpu
from jax.sharding import PartitionSpec as P

CAP = 2
CORES = 2
LINE = 4
LANES = 128
AXES = ("ice", "ocn")
SPAN = 256


def order(count, calls):
    steps = []
    for h in range(count):
        for place, call in zip((0, 1, 4, 7, 12, 16, 22), calls):
            steps.append((3 * h + place, h, call))
    return [step[1:] for step in sorted(steps, key=lambda step: step[:2])]


def kernel(
    sizes, parts,
    route_ref, tiles_ref, valid_ref, rate_ref, land_hbm, ice_hbm, ocean_hbm, w_hbm,
    ice_out, flux_out,
    w_in, wsend, wall, tabv, tabs, namv, nams, rates, res, fres, sea, psend, prec,
    ice_g, fb, own, dsend, drec, zsend, zrec, zrel, csend, crec, mine,
    wl, tl, nl, ns_s, ns_r, ws_s, ws_r, ps_s, ps_r, as_s, as_r, ds_s, ds_r, zs_s, zs_r, rl_s, rl_r,
    fs_s, fs_r, fr_s, gs_s, gs_r, cs_s, cs_r, land_ref, ice_in, ocean_in, il,
):
    X, Y, Z, tiles, blocks = sizes
    Q = X * Y
    H = len(parts)
    per = CORES * CAP
    slots = Z * per
    outer = Z * Y
    cats, fields = rate_ref.shape
    ice_id, ocn_id = lax.axis_index("ice"), lax.axis_index("ocn")
    x, c = ice_id // CORES, ice_id % CORES
    z, y = ocn_id // Y, ocn_id % Y
    side = z // (Z // 2)
    zord = ((Z - 1) * (1 - side), Z // 2 - side, z + 1 - 2 * (z % 2), z)
    is_end = z == (Z - 1) * side
    is_mid = z != (Z - 1) * side

    def chip(j, back=False):
        dx, dy = j // Y, j % Y
        if back:
            dx, dy = X - dx, Y - dy
        return {"ice": ((x + dx) % X) * CORES + c, "ocn": z * Y + (y + dy) % Y}

    partner = {"ice": x * CORES + 1 - c, "ocn": ocn_id}

    def line(zt):
        return {"ice": ice_id, "ocn": zt * Y + y}

    def remote(src, dst, s, r, dev):
        return pltpu.make_async_remote_copy(
            src_ref=src, dst_ref=dst, send_sem=s, recv_sem=r,
            device_id=dev, device_id_type=pl.DeviceIdType.MESH,
        )

    wload = pltpu.make_async_copy(w_hbm, w_in, wl)
    loads = [
        pltpu.make_async_copy(src, dst, il.at[i])
        for i, (src, dst) in enumerate(((land_hbm, land_ref), (ice_hbm, ice_in), (ocean_hbm, ocean_in)))
    ]
    for load in loads:
        load.start()
    wload.start()

    hops = {j: min(j // Y, X - j // Y) + min(j % Y, Y - j % Y) for j in range(Q)}
    near = sorted(range(1, Q), key=hops.get)

    barrier = pltpu.get_barrier_semaphore()
    for j in range(1, Q):
        pl.semaphore_signal(barrier, inc=1, device_id=chip(j), device_id_type=pl.DeviceIdType.MESH)
    for i in range(1, Z):
        pl.semaphore_signal(barrier, inc=1, device_id=line((z + i) % Z), device_id_type=pl.DeviceIdType.MESH)
    pl.semaphore_signal(barrier, inc=1, device_id=partner, device_id_type=pl.DeviceIdType.MESH)

    def acopy(h, j):
        return remote(ice_g[h].at[0], ice_g[h].at[j], as_s.at[h], as_r.at[h], chip(j))

    def ncopy(j):
        return remote(namv.at[j], namv.at[Q + j], ns_s.at[j], ns_r.at[j], chip(j))

    def wcopy(j):
        return remote(wsend.at[j], wall.at[j], ws_s.at[j], ws_r.at[j], chip(j))

    def pcopy(h, g, j):
        at = pl.ds(zord[g] * per, per)
        return remote(psend[h].at[j, at], prec[h].at[j, at], ps_s.at[h, g], ps_r.at[h, g], chip(j))

    others = pl.ds(1, Q - 1)

    def every(src, dst, s, r):
        return remote(src, dst, s, r, partner)

    def pall(h, g):
        at = pl.ds(zord[g] * per, per)
        return every(psend[h].at[others, at], prec[h].at[others, at], ps_s.at[h, g], ps_r.at[h, g])

    def aall(h):
        return every(ice_g[h].at[others], ice_g[h].at[others], as_s.at[h], as_r.at[h])

    def call(h):
        return every(csend[h].at[others], crec[h].at[others], cs_s.at[h], cs_r.at[h])

    def gall(h):
        return every(fb[h].at[c], fb[h].at[1 - c], gs_s.at[h], gs_r.at[h])

    def dall(h):
        return every(dsend[h], drec[h], ds_s.at[h], ds_s.at[h])

    def dcopy(h, zd):
        return remote(dsend[h].at[zd], drec[h].at[zd], ds_s.at[h], ds_r.at[h, zd], partner)

    def zcopy(h, zd):
        return remote(zsend[h].at[zd], zrec[h].at[z], zs_s.at[h, zd], zs_r.at[h, z], line(zd))

    def zwait(h, zs):
        remote(zsend[h].at[zs], zrec[h].at[zs], zs_s.at[h, zs], zs_r.at[h, zs], line(zs)).wait_recv()

    def rcopy(h, g):
        return remote(zsend[h].at[zord[g]], zrel[h].at[g], rl_s.at[h, g], rl_r.at[h, g], line(zord[2]))

    def fcopy(h, zt):
        return remote(fb[h].at[c, z], fb[h].at[c, z], fs_s.at[h, zt], fs_r.at[h, z], line(zt))

    def fwait(h, zs):
        remote(fb[h].at[c, zs], fb[h].at[c, zs], fs_s.at[h, zs], fs_r.at[h, zs], line(zs)).wait_recv()

    def frelay(h, g):
        held = fb[h].at[c, zord[g]]
        return remote(held, held, fr_s.at[h, g], fs_r.at[h, zord[g]], line(zord[2]))

    def gcopy(h, zs):
        return remote(fb[h].at[c, zs], fb[h].at[c, zs], gs_s.at[h], gs_r.at[h], partner)

    def ccopy(h, j):
        return remote(csend[h].at[j], crec[h].at[j], cs_s.at[h], cs_r.at[h], chip(j, True))

    def lanes(t):
        return pl.ds(t * LANES, LANES)

    def land(t):
        return land_ref[pl.ds(t, 1), :].astype(jnp.float32)

    tall = -(-Q // 8) * 8
    sub = lax.broadcasted_iota(jnp.int32, (tall, LANES), 0)
    lane = lax.broadcasted_iota(jnp.int32, (tall, LANES), 1)
    base = jnp.zeros((tall, LANES), jnp.int32)
    for j in range(Q):
        dx, dy = j // Y, j % Y
        own_base = ((x + dx) % X) * CORES * outer + (y + dy) % Y
        base = jnp.where(sub == j, own_base, base)
    turn_of = lane & (CAP - 1)
    core_of = lax.shift_right_logical(lane, CAP.bit_length() - 1) & (CORES - 1)
    line_of = lax.shift_right_logical(lane, per.bit_length() - 1)
    dest = base + core_of * outer + line_of * Y

    def enter(b, carry):
        seen, code, name = carry
        hit = dest == route_ref[0, b]
        take = hit & (seen == turn_of)
        label = tiles_ref[0, b] * tiles + tiles_ref[1, b]
        code = jnp.where(take, (b * SPAN + valid_ref[b]) * (tiles * tiles) + label, code)
        name = jnp.where(take, label, name)
        return seen + jnp.where(hit, 1, 0), code, name

    none = jnp.zeros((tall, LANES), jnp.int32)
    unused, code, name = lax.fori_loop(0, blocks, enter, (none, none, none), unroll=8)
    for j in range(Q):
        tabv[j] = code[j : j + 1, :]
        namv[j] = name[j : j + 1, :]
    tload = pltpu.make_async_copy(tabv, tabs, tl)
    tload.start()

    for load in loads:
        load.wait()
    chans, padded = cats * fields, rates.shape[0]
    for t in range(tiles):
        if chans < padded:
            spare = jnp.zeros((8, LANES), jnp.float32)
            res[t, pl.ds(padded - 8, 8), :] = spare
            sea[t, pl.ds(padded - 8, 8), :] = spare
        for r in range(cats):
            at = pl.ds(r * fields, fields)
            res[t, at, :] = ice_in[r, :, lanes(t)].astype(jnp.float32) * land(t)
            sea[t, at, :] = ocean_in[r, :, lanes(t)].astype(jnp.float32)
    if chans < padded:
        rates[pl.ds(padded - 8, 8), :] = jnp.zeros((8, LANES), jnp.float32)
    for h, (first, count) in enumerate(parts):
        for t in range(tiles):
            ice_g[h][0, t] = res[t, pl.ds(first, count), :].astype(jnp.bfloat16)

    pl.semaphore_wait(barrier, Q - 1 + Z - 1 + 1)
    for j in range(1, Q):
        ncopy(j).start()
    nload = [
        pltpu.make_async_copy(namv.at[j if j == 0 else Q + j], nams.at[j], nl.at[j]) for j in range(Q)
    ]
    nload[0].start()
    tload.wait()
    wload.wait()

    rows = lax.broadcasted_iota(jnp.int32, (LANES, LANES), 0)

    def block(j, n):
        v = tabs[j, 0, n] // (tiles * tiles)
        held = w_in[v // SPAN]
        return jnp.where(rows < v % SPAN, held, jnp.zeros((), jnp.bfloat16))

    def products(h, j, n, held):
        v = tabs[j, 0, n] % (tiles * tiles)
        prod = jnp.dot(ice_g[h][0, v // tiles], held, preferred_element_type=jnp.float32)
        return prod.astype(jnp.bfloat16)

    for g in range(Z):
        def put(i, carry):
            j = Q - 1 - i
            for k in range(per):
                n = zord[g] * per + k
                held = block(j, n)
                wsend[j, n] = held
                for h in range(H):
                    psend[h][j, n] = products(h, j, n, held)
            for h in range(H):
                pcopy(h, g, j).start()
            return carry

        lax.fori_loop(0, Q - 1, put, 0)
    for j in near:
        wcopy(j).start()

    def keep(zd, carry):
        for k in range(per):
            n = zd * per + k
            held = block(0, n)
            wall[0, n] = held
            for h in range(H):
                prec[h][0, n] = products(h, 0, n, held)
        return carry

    lax.fori_loop(0, Z, keep, 0)
    for r in range(cats):
        for f in range(fields):
            rates[pl.ds(r * fields + f, 1), :] = jnp.full((1, LANES), rate_ref[r, f], jnp.float32)
    for j in range(1, Q):
        ncopy(j).wait_recv()
        nload[j].start()
    for j in range(Q):
        nload[j].wait()

    def spread(count, index, prod, accs):
        at = jnp.full((count, LANES), index, jnp.int32)
        return tuple(accs[t] + jnp.where(at == t, prod, 0.0) for t in range(tiles))

    def forward(h, zd, ready=False):
        count = parts[h][1]
        start = tuple(jnp.zeros((count, LANES), jnp.float32) for t in range(tiles))

        def sums(core):
            def add(j, accs):
                for k in range(CAP):
                    n = zd * per + core * CAP + k
                    v = nams[j, 0, n]
                    if ready:
                        prod = prec[h][j, n].astype(jnp.float32)
                    else:
                        prod = jnp.dot(ice_g[h][j, v // tiles], wall[j, n], preferred_element_type=jnp.float32)
                    accs = spread(count, v % tiles, prod, accs)
                return accs

            return lax.fori_loop(0, Q, add, start, unroll=min(Q, 4))

        accs = sums(1 - c)
        for t in range(tiles):
            dsend[h][zd, t] = accs[t].astype(jnp.bfloat16)
        dcopy(h, zd).start()
        accs = sums(c)
        for t in range(tiles):
            own[h][zd, t] = accs[t]

    def merge(h, g):
        zd = zord[g]
        dcopy(h, zd).wait_recv()

        def put():
            for t in range(tiles):
                zsend[h][zd, t] = (own[h][zd, t] + drec[h][zd, t].astype(jnp.float32)).astype(jnp.bfloat16)

        if g < 2:
            @pl.when(is_end)
            def _():
                put()
                rcopy(h, g).start()
        elif g == 2:
            put()
            zcopy(h, zd).start()

    def relay(h, which=(0, 1)):
        @pl.when(is_mid)
        def _():
            for g in which:
                zd = zord[g]
                rcopy(h, g).wait_recv()
                for t in range(tiles):
                    acc = own[h][zd, t] + drec[h][zd, t].astype(jnp.float32) + zrel[h][g, t].astype(jnp.float32)
                    zsend[h][zd, t] = acc.astype(jnp.bfloat16)
                zcopy(h, zd).start()

    def flux(h):
        first, count = parts[h]
        zwait(h, zord[2])
        zwait(h, zord[1])
        for t in range(tiles):
            acc = own[h][z, t] + drec[h][z, t].astype(jnp.float32)
            for g in (2, 1):
                acc = acc + zrec[h][zord[g], t].astype(jnp.float32)
            acc = jnp.tanh(acc + sea[t, pl.ds(first, count), :])
            fb[h][c, z, t] = acc.astype(jnp.bfloat16)
            fres[t, pl.ds(first, count), :] = acc

        fcopy(h, zord[1]).start()
        fcopy(h, zord[2]).start()
        gcopy(h, z).start()

    def arrivals(h):
        def take(g):
            fwait(h, zord[g])
            gcopy(h, zord[g]).start()

        @pl.when(is_mid)
        def _():
            for g in (1, 0):
                fwait(h, zord[g])
                frelay(h, g).start()
                gcopy(h, zord[g]).start()
            take(2)

        @pl.when(is_end)
        def _():
            for g in (2, 1, 0):
                take(g)

    def back(h, j):
        count = parts[h][1]
        accs = tuple(jnp.zeros((count, LANES), jnp.float32) for t in range(tiles))
        for n in range(slots):
            zd, core = n // per, n // CAP % CORES
            v = nams[j, 0, n]
            prod = lax.dot_general(
                fb[h][core, zd, v % tiles], wall[j, n], (((1,), (1,)), ((), ())),
                preferred_element_type=jnp.float32,
            )
            accs = spread(count, v // tiles, prod, accs)
        return accs

    def fluxes(h):
        gall(h).wait_recv()

    def give(h, j):
        accs = back(h, j)
        for t in range(tiles):
            csend[h][j, t] = accs[t].astype(jnp.bfloat16)
        ccopy(h, j).start()

    def hold(h):
        accs = back(h, 0)
        for t in range(tiles):
            mine[h][t] = accs[t]

    def backward(h):
        fluxes(h)

        def one(i, carry):
            give(h, Q - 1 - i)
            return carry

        lax.fori_loop(0, Q - 1, one, 0)
        hold(h)

    def finish(h, number):
        first, count = parts[h]
        call(h).wait_recv()
        if number:
            aall(h).wait_send()
        rate = rates[pl.ds(first, count), :]
        for t in range(tiles):
            acc = mine[h][t]
            for j in range(1, Q):
                acc = acc + crec[h][j, t].astype(jnp.float32)
            old = ice_g[h][0, t].astype(jnp.float32)
            new = land(t) * (old + rate * jnp.tanh(acc))
            if number:
                res[t, pl.ds(first, count), :] = new
            else:
                ice_g[h][0, t] = new.astype(jnp.bfloat16)
        if not number:
            for j in range(Q - 1, 0, -1):
                acopy(h, j).start()

        call(h).wait_send()
        dall(h).wait_send()
        gall(h).wait_send()
        zcopy(h, zord[2]).wait_send()
        for g in (1, 2):
            fcopy(h, zord[g]).wait_send()

        @pl.when(is_end)
        def _():
            for g in range(2):
                rcopy(h, g).wait_send()

        @pl.when(is_mid)
        def _():
            for g in range(2):
                zcopy(h, zord[g]).wait_send()
                frelay(h, g).wait_send()

    def arrive(h):
        aall(h).wait_recv()

    def again(h):
        arrive(h)

        def one(zd, carry):
            forward(h, zd)
            return carry

        lax.fori_loop(0, Z, one, 0)

    def merges(h):
        for g in range(Z):
            merge(h, g)

    for g in range(Z):
        for h in range(H):
            pall(h, g).wait_recv()
            forward(h, zord[g], True)
        for h in range(H):
            merge(h, g)
        if 0 < g < 3:
            for h in range(H):
                relay(h, (g - 1,))
    for h in range(H):
        flux(h)

    def rest(h):
        def one(i, carry):
            give(h, Q - 1 - i)
            return carry

        fluxes(h)
        lax.fori_loop(0, Q - 1, one, 0)
        hold(h)

    last_near = len(near) - max(1, Q // 4)
    for h in range(2):
        arrivals(h)
    fluxes(0)
    for j in near[:last_near]:
        wcopy(j).wait_recv()
        give(0, j)
    for h in range(2, H):
        arrivals(h)
    for j in near[last_near:]:
        wcopy(j).wait_recv()
        give(0, j)
    hold(0)
    for h in range(1, H):
        rest(h)
        finish(h - 1, 0)
    again(0)
    merges(0)
    finish(H - 1, 0)
    for j in range(1, Q):
        wcopy(j).wait_send()
        ncopy(j).wait_send()
    for h in range(H):
        for g in range(Z):
            pall(h, g).wait_send()

    def send(r, held, out):
        for t in range(tiles):
            out[r, :, lanes(t)] = held[t, pl.ds(r * fields, fields), :].astype(jnp.bfloat16)

    def last(h):
        if h == H - 1:
            for r in range(cats):
                send(r, fres, flux_out)
        finish(h, 1)
        first, count = parts[h]
        for r in range(cats):
            if first < (r + 1) * fields <= first + count:
                send(r, res, ice_out)

    for h, step in order(H, (again, merges, relay, flux, arrivals, backward, last)):
        if h or step not in (again, merges):
            step(h)


def cut(chans):
    rows = -(-chans // 8) * 8
    sizes = [32] * (rows // 32 - 1)
    sizes.append(rows - sum(sizes))
    parts, first = [], 0
    for size in sizes:
        parts.append((first, size))
        first += size
    return tuple(parts)


def on_device(
    ice_state, ocean_state, ice_rate, block_weights, block_route, block_tiles, block_valid, ice_mask
):
    cats, fields, cells = ice_state.shape
    chans = cats * fields
    blocks, width, unused = block_weights.shape
    tiles = cells // width
    outer = lax.axis_size("ocn")
    Z = LINE
    Y = outer // Z
    X = lax.axis_size("ice") // CORES
    Q = X * Y
    slots = Z * CORES * CAP
    assert outer % LINE == 0
    parts = cut(chans)
    H = len(parts)
    rows = sum(part[1] for part in parts)

    def each(*lead, dtype=jnp.bfloat16):
        return tuple(pltpu.VMEM(lead + (part[1], width), dtype) for part in parts)

    def sems(*shape):
        return pltpu.SemaphoreType.DMA(shape)

    smem, vmem = pl.BlockSpec(memory_space=pltpu.SMEM), pl.BlockSpec(memory_space=pltpu.VMEM)
    ice, flux = pl.pallas_call(
        functools.partial(kernel, (X, Y, Z, tiles, blocks), parts),
        out_shape=(jax.ShapeDtypeStruct(ice_state.shape, jnp.bfloat16),) * 2,
        in_specs=[smem] * 4 + [pl.BlockSpec(memory_space=pltpu.HBM)] * 4,
        out_specs=(vmem, vmem),
        scratch_shapes=[
            pltpu.VMEM((blocks, width, width), jnp.bfloat16),
            pltpu.VMEM((Q, slots, width, width), jnp.bfloat16),
            pltpu.VMEM((Q, slots, width, width), jnp.bfloat16),
            pltpu.VMEM((Q, 1, width), jnp.int32),
            pltpu.SMEM((Q, 1, width), jnp.int32),
            pltpu.VMEM((2 * Q, 1, width), jnp.int32),
            pltpu.SMEM((Q, 1, width), jnp.int32),
            pltpu.VMEM((rows, width), jnp.float32),
            pltpu.VMEM((tiles, rows, width), jnp.float32),
            pltpu.VMEM((tiles, rows, width), jnp.float32),
            pltpu.VMEM((tiles, rows, width), jnp.float32),
            each(Q, slots),
            each(Q, slots),
            each(Q, tiles),
            each(CORES, Z, tiles),
            each(Z, tiles, dtype=jnp.float32),
            each(Z, tiles),
            each(Z, tiles),
            each(Z, tiles),
            each(Z, tiles),
            each(2, tiles),
            each(Q, tiles),
            each(Q, tiles),
            each(tiles, dtype=jnp.float32),
            pltpu.SemaphoreType.DMA,
            pltpu.SemaphoreType.DMA,
            sems(Q), sems(Q), sems(Q),
            sems(Q), sems(Q),
            sems(H, Z), sems(H, Z),
            sems(H), sems(H),
            sems(H), sems(H, Z),
            sems(H, Z), sems(H, Z),
            sems(H, 2), sems(H, 2),
            sems(H, Z), sems(H, Z),
            sems(H, 2),
            sems(H), sems(H),
            sems(H), sems(H),
            pltpu.VMEM((tiles, width), jnp.int32),
            pltpu.VMEM(ice_state.shape, jnp.bfloat16),
            pltpu.VMEM(ice_state.shape, jnp.bfloat16),
            sems(3),
        ],
        compiler_params=pltpu.CompilerParams(
            collective_id=0, has_side_effects=True, vmem_limit_bytes=60 * 1024 * 1024
        ),
    )(
        block_route.T, block_tiles.T, block_valid, ice_rate, ice_mask.reshape(tiles, width),
        ice_state, ocean_state, block_weights,
    )
    return ice, flux


def solution(mesh):
    placed = (
        P(None, None, AXES), P(None, None, AXES), P(), P(AXES, None, None),
        P(AXES, None), P(AXES, None), P(AXES), P(AXES),
    )
    return jax.shard_map(
        on_device, mesh=mesh, in_specs=placed,
        out_specs=(P(None, None, AXES), P(None, None, AXES)), check_vma=False,
    )
```
